16 devices in a mesh: dp: 16 (over z, y, x, core).
Axes of the slice: x: 2, y: 2, z: 2, core: 2. Of those that a mesh axis runs over, the one named last changes fastest.
Arguments:
- img_emb: bfloat16 [32768, 768], P('dp')
- txt_emb: bfloat16 [32768, 768], P('dp')
- log_temp: float32 [1], replicated
- logit_bias: float32 [1], replicated
Outputs:
- output 1: float32 [1], replicated
- output 2: float32 [32768, 768], P('dp')
- output 3: float32 [32768, 768], P('dp')
- output 4: float32 [1], replicated
- output 5: float32 [1], replicated
All inputs are finite; a program needn't handle non-finite values.
Results may differ from the reference program's by a relative error of at most 0.001.
Values are sent between devices in bfloat16 or wider.
A program may use at most 1 GiB of HBM per device.

```python
import math
import jax
import jax.numpy as jnp
from jax import lax

ROWS = 2048
DEVICES = 16
EMBED = 768
ROW_BLOCK = 64


def setup_inputs(seed: int = 0) -> dict:
    n_total = ROWS * DEVICES
    sub_keys = jax.random.split(jax.random.key(seed), 6)
    latent = jax.random.normal(sub_keys[0], (n_total, EMBED), jnp.float32)
    shard_shift = jax.random.randint(sub_keys[1], (n_total,), 1, DEVICES)
    partner = (jnp.arange(n_total) + shard_shift * ROWS) % n_total
    img_raw = latent + 0.5 * jax.random.normal(sub_keys[2], (n_total, EMBED), jnp.float32)
    txt_raw = latent + 0.8 * latent[partner] + 0.5 * jax.random.normal(sub_keys[3], (n_total, EMBED), jnp.float32)
    img_emb = img_raw / jnp.linalg.norm(img_raw, axis=1, keepdims=True)
    txt_emb = txt_raw / jnp.linalg.norm(txt_raw, axis=1, keepdims=True)
    log_temp = math.log(2.0 * math.log(n_total)) + jax.random.uniform(sub_keys[4], (1,), jnp.float32, -0.25, 0.25)
    logit_bias = -math.log(n_total) + jax.random.uniform(sub_keys[5], (1,), jnp.float32, -1.0, 1.0)
    return {'img_emb': img_emb.astype(jnp.bfloat16), 'txt_emb': txt_emb.astype(jnp.bfloat16), 'log_temp': log_temp, 'logit_bias': logit_bias}


def reference(img_emb, txt_emb, log_temp, logit_bias):
    n_total = img_emb.shape[0]
    n_blocks = n_total // ROW_BLOCK
    temp_scale = jnp.exp(log_temp[0])
    bias_val = logit_bias[0]
    col_ids = jnp.arange(n_total)
    img_blocks = img_emb.reshape(n_blocks, ROW_BLOCK, EMBED)

    def block_step(loop_state, step_in):
        loss_acc, bias_acc, temp_acc, txt_acc = loop_state
        block_idx, img_block = step_in
        row_ids = block_idx * ROW_BLOCK + jnp.arange(ROW_BLOCK)
        labels = jnp.where(row_ids[:, None] == col_ids[None, :], 1.0, -1.0)
        dot_vals = jnp.dot(img_block, txt_emb.T, preferred_element_type=jnp.float32)
        margin = labels * (temp_scale * dot_vals + bias_val)
        loss_acc = loss_acc + jnp.sum(jax.nn.softplus(-margin))
        grad_coef = -labels * jax.nn.sigmoid(-margin)
        coef_bf16 = grad_coef.astype(jnp.bfloat16)
        bias_acc = bias_acc + jnp.sum(grad_coef)
        temp_acc = temp_acc + jnp.sum(grad_coef * dot_vals)
        img_part = jnp.dot(coef_bf16, txt_emb, preferred_element_type=jnp.float32)
        txt_acc = txt_acc + jnp.dot(coef_bf16.T, img_block, preferred_element_type=jnp.float32)
        return (loss_acc, bias_acc, temp_acc, txt_acc), img_part

    zero_val = jnp.zeros((), jnp.float32)
    init_state = (zero_val, zero_val, zero_val, jnp.zeros((n_total, EMBED), jnp.float32))
    final_state, img_parts = lax.scan(block_step, init_state, (jnp.arange(n_blocks), img_blocks))
    loss_acc, bias_acc, temp_acc, txt_acc = final_state
    factor = temp_scale / n_total
    total_loss = (loss_acc / n_total).reshape(1)
    img_grad = img_parts.reshape(n_total, EMBED) * factor
    txt_grad = txt_acc * factor
    temp_grad = (temp_acc * factor).reshape(1)
    bias_grad = (bias_acc / n_total).reshape(1)
    return (total_loss, img_grad, txt_grad, temp_grad, bias_grad)
```

```python
import jax
import jax.numpy as jnp
from jax import lax
from jax.experimental import pallas as pl
from jax.experimental.pallas import tpu as pltpu
from jax.sharding import PartitionSpec as P

LOG2E = 1.4426950408889634
LN2 = 0.6931471805599453
BQ = 1024
BK = 512
CLAMP = 30.0
NT = (((1,), (1,)), ((), ()))
NN = (((1,), (0,)), ((), ()))


def fold(z):
    rows, cols = z.shape
    if cols > 128:
        z = sum(z[:, c:c + 128] for c in range(0, cols, 128))
    return jnp.sum(z.reshape(rows // 8, 8, 128), axis=0)


def log_one_plus(x):
    w = 1.0 + x
    return jnp.log(w) + jnp.where(x < 1.0, x - (w - 1.0), 0.0)


def pair_terms(tx, ty):
    ex, ey = jnp.exp2(tx), jnp.exp2(ty)
    ay = 1.0 + ey
    w = ex * ay
    q = w + ey
    d = 1.0 + q
    r = 1.0 / d
    return w * r, (ey * (1.0 + ex)) * r, q, d


def logits(s_ref, k, a, b2, offset):
    quarter = BK // 4
    dot = s_ref[:, k * quarter:(k + 1) * quarter]
    t = a * dot + b2
    if offset is None:
        return dot, t, None
    rows = lax.broadcasted_iota(jnp.int32, dot.shape, 0)
    cols = lax.broadcasted_iota(jnp.int32, dot.shape, 1) + k * quarter
    match = rows - cols == offset
    return dot, jnp.where(match, -t, t), match


def img_elem(s_ref, c_ref, sums_ref, a, b2, offset):
    quarter = BK // 4
    dots, ts, matches = zip(*[logits(s_ref, k, a, b2, offset) for k in range(4)])
    tc = [jnp.minimum(t, CLAMP) for t in ts]
    p0, p1, q01, _ = pair_terms(tc[0], tc[1])
    p2, p3, q23, d23 = pair_terms(tc[2], tc[3])
    ps = [p0, p1, p2, p3]
    if offset is not None:
        ps = [jnp.where(m, -p, p) for m, p in zip(matches, ps)]
    q4 = q01 * d23 + q23
    over = [t - c for t, c in zip(ts, tc)]
    sums_ref[0] += fold(log_one_plus(q4) + LN2 * ((over[0] + over[1]) + (over[2] + over[3])))
    sums_ref[1] += fold((ps[0] + ps[1]) + (ps[2] + ps[3]))
    sums_ref[2] += fold((ps[0] * dots[0] + ps[1] * dots[1]) + (ps[2] * dots[2] + ps[3] * dots[3]))
    for k in range(4):
        c_ref[:, k * quarter:(k + 1) * quarter] = ps[k].astype(jnp.bfloat16)


def txt_elem(s_ref, c_ref, a, b2, offset):
    quarter = BK // 4
    for k in range(0, 4, 2):
        _, tx, mx = logits(s_ref, k, a, b2, offset)
        _, ty, my = logits(s_ref, k + 1, a, b2, offset)
        px, py, _, _ = pair_terms(jnp.minimum(tx, 2 * CLAMP), jnp.minimum(ty, 2 * CLAMP))
        if offset is not None:
            px, py = jnp.where(mx, -px, px), jnp.where(my, -py, py)
        c_ref[:, k * quarter:(k + 1) * quarter] = px.astype(jnp.bfloat16)
        c_ref[:, (k + 1) * quarter:(k + 2) * quarter] = py.astype(jnp.bfloat16)


def kernel(coef, q0_ref, q1_ref, k0_ref, k1_ref, out0_ref, out1_ref, sums_ref, kb0, kb1, s00, s01, s10, s11, c00, c01, c10, c11, ksem):
    nkb = k0_ref.shape[0] // BK
    rows_local = q0_ref.shape[0]
    nq = rows_local // BQ
    own_steps = (rows_local // BK) * nq
    total = nkb * nq
    a, b2 = coef[0], coef[1]
    me = lax.axis_index('dp')

    def fetch(j):
        sl = lax.rem(j, 3)
        row = pl.multiple_of(lax.rem(me * rows_local + j * BK, k0_ref.shape[0]), BK)
        return [pltpu.make_async_copy(k.at[pl.ds(row, BK), :], kb.at[sl], ksem.at[i, sl]) for i, (k, kb) in enumerate(((k0_ref, kb0), (k1_ref, kb1)))]

    sums_ref[...] = jnp.zeros_like(sums_ref)
    out0_ref[...] = jnp.zeros_like(out0_ref)
    out1_ref[...] = jnp.zeros_like(out1_ref)
    c01[...] = jnp.zeros_like(c01)
    c11[...] = jnp.zeros_like(c11)
    for c in fetch(0) + fetch(1):
        c.start()
    for c in fetch(0):
        c.wait()
    s00[...] = lax.dot_general(q0_ref[0:BQ, :], kb0[0], NT, preferred_element_type=jnp.float32)
    s10[...] = lax.dot_general(q1_ref[0:BQ, :], kb1[0], NT, preferred_element_type=jnp.float32)

    def grads(qp, sp, o, ci, kb):
        o[pl.ds(qp, BQ), :] += lax.dot_general(ci[...], kb[sp], NN, preferred_element_type=jnp.float32)

    def step(t, s0i, s0o, s1i, s1o, c0i, c0o, c1i, c1o, own):
        t_next = jnp.minimum(t + 1, total - 1)
        t_prev = jnp.maximum(t - 1, 0)
        qn = pl.multiple_of(lax.rem(t_next, nq) * BQ, BQ)
        qp = pl.multiple_of(lax.rem(t_prev, nq) * BQ, BQ)
        sn = lax.rem(lax.div(t_next, nq), 3)
        sp = lax.rem(lax.div(t_prev, nq), 3)
        offset = lax.div(t, nq) * BK - lax.rem(t, nq) * BQ if own else None
        s0o[...] = lax.dot_general(q0_ref[pl.ds(qn, BQ), :], kb0[sn], NT, preferred_element_type=jnp.float32)
        img_elem(s0i, c0o, sums_ref, a, b2, offset)
        grads(qp, sp, out0_ref, c0i, kb0)
        s1o[...] = lax.dot_general(q1_ref[pl.ds(qn, BQ), :], kb1[sn], NT, preferred_element_type=jnp.float32)
        txt_elem(s1i, c1o, a, b2, offset)
        grads(qp, sp, out1_ref, c1i, kb1)

    def body(own):
        def run(h, _):
            j = h

            @pl.when(j + 1 < nkb)
            def _():
                for c in fetch(j + 1):
                    c.wait()

            step(2 * h, s00, s01, s10, s11, c01, c00, c11, c10, own)

            @pl.when(j + 2 < nkb)
            def _():
                for c in fetch(j + 2):
                    c.start()

            step(2 * h + 1, s01, s00, s11, s10, c00, c01, c10, c11, own)
            return 0
        return run

    lax.fori_loop(0, own_steps // 2, body(True), 0)
    lax.fori_loop(own_steps // 2, total // 2, body(False), 0)
    grads((nq - 1) * BQ, (nkb - 1) % 3, out0_ref, c01, kb0)
    grads((nq - 1) * BQ, (nkb - 1) % 3, out1_ref, c11, kb1)


def both_sides(coef, q0, q1, k0, k1):
    rows, depth = q0.shape
    in_vmem = pl.BlockSpec(memory_space=pltpu.VMEM)
    anywhere = pl.BlockSpec(memory_space=pl.ANY)
    grad = jax.ShapeDtypeStruct((rows, depth), jnp.float32)
    return pl.pallas_call(
        kernel,
        out_shape=(grad, grad, jax.ShapeDtypeStruct((3, 8, 128), jnp.float32)),
        in_specs=[pl.BlockSpec(memory_space=pltpu.SMEM), in_vmem, in_vmem, anywhere, anywhere],
        out_specs=(in_vmem, in_vmem, in_vmem),
        scratch_shapes=[pltpu.VMEM((3, BK, depth), jnp.bfloat16)] * 2
        + [pltpu.VMEM((BQ, BK), jnp.float32)] * 4
        + [pltpu.VMEM((BQ, BK), jnp.bfloat16)] * 4
        + [pltpu.SemaphoreType.DMA((2, 3))],
        compiler_params=pltpu.CompilerParams(vmem_limit_bytes=62 * 1024 * 1024),
    )(coef, q0, q1, k0, k1)


def solution(mesh):
    axis_name = mesh.axis_names[0]
    n_dev = mesh.shape[axis_name]

    def per_device(img, txt, log_temp, logit_bias):
        n_total = img.shape[0] * n_dev
        scale = jnp.exp(log_temp[0])
        coef = jnp.stack([scale * LOG2E, logit_bias[0] * LOG2E])
        txt_all = lax.all_gather(txt, axis_name, tiled=True)
        img_all = lax.all_gather(img, axis_name, tiled=True)
        img_sum, txt_sum, sums = both_sides(coef, img, txt, txt_all, img_all)
        factor = scale / n_total
        totals = lax.psum(jnp.sum(sums, axis=(1, 2)), axis_name)
        return totals[0:1] / n_total, img_sum * factor, txt_sum * factor, totals[2:3] * factor, totals[1:2] / n_total

    return jax.shard_map(per_device, mesh=mesh, in_specs=(P(axis_name, None), P(axis_name, None), P(None), P(None)), out_specs=(P(None), P(axis_name, None), P(axis_name, None), P(None), P(None)), check_vma=False)
```

```python
import jax
import jax.numpy as jnp
from jax import lax
from jax.experimental import pallas as pl
from jax.experimental.pallas import tpu as pltpu
from jax.sharding import PartitionSpec as P

LOG2E = 1.4426950408889634
LN2 = 0.6931471805599453
BQ = 1024
BK = 512
CLAMP = 30.0
NT = (((1,), (1,)), ((), ()))
NN = (((1,), (0,)), ((), ()))


def fold(z):
    rows, cols = z.shape
    if cols > 128:
        z = sum(z[:, c:c + 128] for c in range(0, cols, 128))
    return jnp.sum(z.reshape(rows // 8, 8, 128), axis=0)


def log_one_plus(x):
    w = 1.0 + x
    return jnp.log(w) + jnp.where(x < 1.0, x - (w - 1.0), 0.0)


def joint(ex, ey):
    return ex * (1.0 + ey) + ey


def logits(s_ref, k, a, b2, offset):
    quarter = BK // 4
    dot = s_ref[:, k * quarter:(k + 1) * quarter]
    t = a * dot + b2
    if offset is None:
        return dot, t, None
    rows = lax.broadcasted_iota(jnp.int32, dot.shape, 0)
    cols = lax.broadcasted_iota(jnp.int32, dot.shape, 1) + k * quarter
    match = rows - cols == offset
    return dot, jnp.where(match, -t, t), match


def img_elem(s_ref, c_ref, sums_ref, a, b2, offset):
    quarter = BK // 4
    dots, ts, matches = zip(*[logits(s_ref, k, a, b2, offset) for k in range(4)])
    tc = [jnp.minimum(t, CLAMP) for t in ts]
    es = [jnp.exp2(t) for t in tc]
    ps = [e * (1.0 / (1.0 + e)) for e in es]
    if offset is not None:
        ps = [jnp.where(m, -p, p) for m, p in zip(matches, ps)]
    q4 = joint(joint(es[0], es[1]), joint(es[2], es[3]))
    over = [t - c for t, c in zip(ts, tc)]
    sums_ref[0] += fold(log_one_plus(q4) + LN2 * ((over[0] + over[1]) + (over[2] + over[3])))
    sums_ref[1] += fold((ps[0] + ps[1]) + (ps[2] + ps[3]))
    sums_ref[2] += fold((ps[0] * dots[0] + ps[1] * dots[1]) + (ps[2] * dots[2] + ps[3] * dots[3]))
    for k in range(4):
        c_ref[:, k * quarter:(k + 1) * quarter] = ps[k].astype(jnp.bfloat16)


def txt_elem(s_ref, c_ref, a, b2, offset):
    quarter = BK // 4
    for k in range(4):
        _, t, match = logits(s_ref, k, -a, -b2, offset)
        p = 1.0 / (1.0 + jnp.exp2(t))
        if offset is not None:
            p = jnp.where(match, -p, p)
        c_ref[:, k * quarter:(k + 1) * quarter] = p.astype(jnp.bfloat16)


def kernel(coef, q0_ref, q1_ref, own0_ref, own1_ref, out0_ref, out1_ref, sums_ref, all0_ref, all1_ref, kb0, kb1, s00, s01, s10, s11, c00, c01, c10, c11, ksem, hop_send, hop_recv, pair_send, pair_recv, part_ref, gathered, sum_send, sum_recv, free):
    rows_local = q0_ref.shape[0]
    nq = rows_local // BQ
    parts = rows_local // BK
    chips = all0_ref.shape[0] // rows_local
    n_dev = 2 * chips
    nkb = n_dev * parts
    total = nkb * nq
    a, b2 = coef[0], coef[1]
    me = lax.axis_index('dp')
    core, chip = lax.rem(me, 2), lax.div(me, 2)
    partner = me + 1 - 2 * core
    owns, alls, kbs, locals_ = (own0_ref, own1_ref), (all0_ref, all1_ref), (kb0, kb1), (q1_ref, q0_ref)

    def remote(source, target, send, recv, device):
        return pltpu.make_async_remote_copy(source, target, send, recv, device_id=(device,), device_id_type=pl.DeviceIdType.MESH)

    def weights(part, side):
        result = []
        for k in range(3):
            axis = jnp.where(part == 3, 2 - k if side == 0 else k, lax.rem(part + k, 3))
            weight = 1 + axis + lax.div(axis, 2)
            result.append(weight * (1 - 2 * lax.rem(lax.div(chip, weight), 2)))
        return result

    def place(route, part, side):
        bits = (lax.rem(route, 2), lax.rem(lax.div(route, 2), 2), lax.div(route, 4))
        source = chip
        for bit, flip in zip(bits, weights(part, side)):
            source = source + bit * flip
        return pl.ds(pl.multiple_of(source * rows_local + part * BK, BK), BK)

    def message(route, part, side):
        return (route * parts + part) * 2 + side

    def local_rows(part, side):
        return locals_[side].at[pl.ds(pl.multiple_of(part * BK, BK), BK), :]

    def hop(route, k, part, side, own=False):
        index = message(route + (1 << k), part, side)
        rows = alls[side].at[place(route, part, side), :]
        return remote(local_rows(part, side) if own else rows, rows, hop_send.at[index], hop_recv.at[index], me + 2 * weights(part, side)[k])

    def hop_arrival(route, part, side):
        index = message(route, part, side)
        rows = alls[side].at[place(route, part, side), :]
        return remote(rows, rows, hop_send.at[index], hop_recv.at[index], partner)

    def pair(route, part, side, source):
        index = message(route, part, side)
        return remote(source, kbs[side].at[3 + part], pair_send.at[index], pair_recv.at[index], partner)

    def stage_of(j):
        return lax.div(j, 2 * parts)

    def route_of(j):
        i = stage_of(j)
        return i + jnp.where(i == 3, 1, 0) - jnp.where(i == 4, 1, 0)

    def part_of(j):
        return lax.rem(j, parts)

    def from_partner(j):
        return lax.rem(lax.div(j, parts), 2) == 1

    def ring(j):
        return lax.rem(stage_of(j) * parts + part_of(j), 3)

    def slot(j):
        return jnp.where(from_partner(j), 3 + part_of(j), ring(j))

    def fetch_own(j):
        row = pl.multiple_of(part_of(j) * BK, BK)
        return [pltpu.make_async_copy(owns[side].at[pl.ds(row, BK), :], kbs[side].at[ring(j)], ksem.at[side, ring(j)]) for side in range(2)]

    def fetch(j):
        return [pltpu.make_async_copy(alls[side].at[place(route_of(j), part_of(j), side), :], kbs[side].at[ring(j)], ksem.at[side, ring(j)]) for side in range(2)]

    def pair_block(j, side):
        return pair(route_of(j), part_of(j), side, kbs[side].at[ring(j)])

    def make_ready(j):
        partner_block = from_partner(j)

        @pl.when(partner_block)
        def _():
            for side in range(2):
                pair_block(j, side).wait_recv()

        @pl.when(jnp.logical_not(partner_block))
        def _():
            for c in fetch(j):
                c.wait()
            pl.semaphore_wait(free.at[part_of(j)], 1)
            for side in range(2):
                pair_block(j, side).start()

    def prefetch(j):
        route, part = route_of(j), part_of(j)
        for side in range(2):
            hop_arrival(route, part, side).wait_recv()
        for k in range(1, 3):
            @pl.when(route < (1 << k))
            def _():
                for side in range(2):
                    hop(route, k, part, side).start()

        @pl.when(stage_of(j) * parts + part - 3 >= parts)
        def _():
            back = jnp.where(part == 3, j - 3, j - 2 * parts + 1)
            for side in range(2):
                pair_block(back, side).wait_send()
        for c in fetch(j):
            c.start()

    barrier = pltpu.get_barrier_semaphore()

    def greet(n, _):
        pl.semaphore_signal(barrier, inc=1, device_id=(lax.rem(me + n, n_dev),), device_id_type=pl.DeviceIdType.MESH)
        return 0

    lax.fori_loop(1, n_dev, greet, 0)
    for c in fetch_own(0) + fetch_own(1):
        c.start()
    pl.semaphore_wait(barrier, n_dev - 1)

    def start_own(part, _):
        for side in range(2):
            hop(0, 0, part, side, own=True).start()
        for side in range(2):
            pair(0, part, side, local_rows(part, side)).start()
        return 0

    def start_later(part, _):
        for k in range(1, 3):
            for side in range(2):
                hop(0, k, part, side, own=True).start()
        return 0

    lax.fori_loop(0, parts, start_own, 0)
    lax.fori_loop(0, parts, start_later, 0)

    part_ref[...] = jnp.zeros_like(part_ref)
    out0_ref[...] = jnp.zeros_like(out0_ref)
    out1_ref[...] = jnp.zeros_like(out1_ref)
    c01[...] = jnp.zeros_like(c01)
    c11[...] = jnp.zeros_like(c11)
    for c in fetch_own(0):
        c.wait()
    s00[...] = lax.dot_general(q0_ref[0:BQ, :], kb0[0], NT, preferred_element_type=jnp.float32)
    s10[...] = lax.dot_general(q1_ref[0:BQ, :], kb1[0], NT, preferred_element_type=jnp.float32)

    def grads(qp, sp, o, ci, kb):
        o[pl.ds(qp, BQ), :] += lax.dot_general(ci[...], kb[sp], NN, preferred_element_type=jnp.float32)

    def step(t, s0i, s0o, s1i, s1o, c0i, c0o, c1i, c1o, own):
        t_next = jnp.minimum(t + 1, total - 1)
        t_prev = jnp.maximum(t - 1, 0)
        qn = pl.multiple_of(lax.rem(t_next, nq) * BQ, BQ)
        qp = pl.multiple_of(lax.rem(t_prev, nq) * BQ, BQ)
        sn = slot(lax.div(t_next, nq))
        sp = slot(lax.div(t_prev, nq))
        offset = lax.div(t, nq) * BK - lax.rem(t, nq) * BQ if own else None
        s0o[...] = lax.dot_general(q0_ref[pl.ds(qn, BQ), :], kb0[sn], NT, preferred_element_type=jnp.float32)
        img_elem(s0i, c0o, part_ref, a, b2, offset)
        grads(qp, sp, out0_ref, c0i, kb0)
        s1o[...] = lax.dot_general(q1_ref[pl.ds(qn, BQ), :], kb1[sn], NT, preferred_element_type=jnp.float32)
        txt_elem(s1i, c1o, a, b2, offset)
        grads(qp, sp, out1_ref, c1i, kb1)

    def own_body(j, _):
        @pl.when(j + 1 < parts)
        def _():
            for c in fetch_own(j + 1):
                c.wait()

        @pl.when(j + 1 == parts)
        def _():
            for side in range(2):
                pair(0, 0, side, local_rows(0, side)).wait_recv()

        step(2 * j, s00, s01, s10, s11, c01, c00, c11, c10, True)

        @pl.when(j + 2 < parts)
        def _():
            for c in fetch_own(j + 2):
                c.start()

        step(2 * j + 1, s01, s00, s11, s10, c00, c01, c10, c11, True)
        return 0

    def body(j, _):
        @pl.when(j + 1 < nkb)
        def _():
            make_ready(j + 1)

        step(2 * j, s00, s01, s10, s11, c01, c00, c11, c10, False)

        @pl.when(jnp.logical_and(from_partner(j - 1), j - 1 < nkb - parts))
        def _():
            pl.semaphore_signal(free.at[part_of(j - 1)], inc=1, device_id=(partner,), device_id_type=pl.DeviceIdType.MESH)

        @pl.when(jnp.logical_and(j + 2 < nkb, jnp.logical_not(from_partner(j + 2))))
        def _():
            prefetch(j + 2)

        step(2 * j + 1, s01, s00, s11, s10, c00, c01, c10, c11, False)
        return 0

    lax.fori_loop(0, parts, own_body, 0)
    lax.fori_loop(parts, nkb, body, 0)
    last = slot(nkb - 1)
    grads((nq - 1) * BQ, last, out0_ref, c01, kb0)

    def share(target, sender):
        return remote(part_ref, gathered.at[sender], sum_send.at[target], sum_recv.at[sender], target)

    def share_start(n, _):
        share(lax.rem(me + n, n_dev), me).start()
        return 0

    def share_wait(n, _):
        other = lax.rem(me + n, n_dev)
        share(other, other).wait_recv()
        share(other, me).wait_send()
        return 0

    lax.fori_loop(1, n_dev, share_start, 0)
    gathered[me] = part_ref[...]
    grads((nq - 1) * BQ, last, out1_ref, c11, kb1)
    lax.fori_loop(1, n_dev, share_wait, 0)
    sums_ref[...] = jnp.sum(gathered[...], axis=0)

    def drain_hops(n, _):
        for side in range(2):
            hop_arrival(lax.div(n, parts), lax.rem(n, parts), side).wait_send()
        return 0

    def drain_first(part, _):
        for side in range(2):
            pair(0, part, side, local_rows(part, side)).wait_send()
        return 0

    def drain_last(part, _):
        for side in range(2):
            pair_block(nkb - 2 * parts + part, side).wait_send()
        return 0

    lax.fori_loop(parts, chips * parts, drain_hops, 0)
    lax.fori_loop(0, parts, drain_first, 0)
    lax.fori_loop(1, parts, drain_last, 0)


def both_sides(coef, img, txt, n_dev):
    rows, depth = img.shape
    in_vmem = pl.BlockSpec(memory_space=pltpu.VMEM)
    anywhere = pl.BlockSpec(memory_space=pl.ANY)
    grad = jax.ShapeDtypeStruct((rows, depth), jnp.float32)
    whole = jax.ShapeDtypeStruct((rows * (n_dev // 2), depth), img.dtype)
    messages = 8 * (rows // BK) * 2
    return pl.pallas_call(
        kernel,
        out_shape=(grad, grad, jax.ShapeDtypeStruct((3, 8, 128), jnp.float32), whole, whole),
        in_specs=[pl.BlockSpec(memory_space=pltpu.SMEM), in_vmem, in_vmem, anywhere, anywhere],
        out_specs=(in_vmem, in_vmem, in_vmem, anywhere, anywhere),
        scratch_shapes=[pltpu.VMEM((3 + rows // BK, BK, depth), jnp.bfloat16)] * 2
        + [pltpu.VMEM((BQ, BK), jnp.float32)] * 4
        + [pltpu.VMEM((BQ, BK), jnp.bfloat16)] * 4
        + [pltpu.SemaphoreType.DMA((2, 3))]
        + [pltpu.SemaphoreType.DMA((messages,))] * 4
        + [pltpu.VMEM((3, 8, 128), jnp.float32), pltpu.VMEM((n_dev, 3, 8, 128), jnp.float32)]
        + [pltpu.SemaphoreType.DMA((n_dev,))] * 2
        + [pltpu.SemaphoreType.REGULAR((rows // BK,))],
        compiler_params=pltpu.CompilerParams(vmem_limit_bytes=62 * 1024 * 1024, collective_id=0, has_side_effects=True),
    )(coef, img, txt, txt, img)


def solution(mesh):
    axis_name = mesh.axis_names[0]
    n_dev = mesh.shape[axis_name]

    def per_device(img, txt, log_temp, logit_bias):
        n_total = img.shape[0] * n_dev
        scale = jnp.exp(log_temp[0])
        coef = jnp.stack([scale * LOG2E, logit_bias[0] * LOG2E])
        img_sum, txt_sum, sums, _, _ = both_sides(coef, img, txt, n_dev)
        factor = scale / n_total
        totals = jnp.sum(sums, axis=(1, 2))
        return totals[0:1] / n_total, img_sum * factor, txt_sum * factor, totals[2:3] * factor, totals[1:2] / n_total

    return jax.shard_map(per_device, mesh=mesh, in_specs=(P(axis_name, None), P(axis_name, None), P(None), P(None)), out_specs=(P(None), P(axis_name, None), P(axis_name, None), P(None), P(None)), check_vma=False)
```

```python
import jax
import jax.numpy as jnp
from jax import lax
from jax.experimental import pallas as pl
from jax.experimental.pallas import tpu as pltpu
from jax.sharding import PartitionSpec as P

LOG2E = 1.4426950408889634
LN2 = 0.6931471805599453
BQ = 1024
BK = 512
CLAMP = 30.0
NT = (((1,), (1,)), ((), ()))
NN = (((1,), (0,)), ((), ()))


def fold(z):
    rows, cols = z.shape
    if cols > 128:
        z = sum(z[:, c:c + 128] for c in range(0, cols, 128))
    return jnp.sum(z.reshape(rows // 8, 8, 128), axis=0)


def log_one_plus(x):
    w = 1.0 + x
    return jnp.log(w) + jnp.where(x < 1.0, x - (w - 1.0), 0.0)


def joint(ex, ey):
    return ex * (1.0 + ey) + ey


def logits(s_ref, k, a, b2, offset):
    quarter = BK // 4
    dot = s_ref[:, k * quarter:(k + 1) * quarter]
    t = a * dot + b2
    if offset is None:
        return dot, t, None
    rows = lax.broadcasted_iota(jnp.int32, dot.shape, 0)
    cols = lax.broadcasted_iota(jnp.int32, dot.shape, 1) + k * quarter
    match = rows - cols == offset
    return dot, jnp.where(match, -t, t), match


def img_elem(s_ref, c_ref, sums_ref, a, b2, offset):
    quarter = BK // 4
    dots, ts, matches = zip(*[logits(s_ref, k, a, b2, offset) for k in range(4)])
    tc = [jnp.minimum(t, CLAMP) for t in ts]
    es = [jnp.exp2(t) for t in tc]
    ps = [e * (1.0 / (1.0 + e)) for e in es]
    if offset is not None:
        ps = [jnp.where(m, -p, p) for m, p in zip(matches, ps)]
    q4 = joint(joint(es[0], es[1]), joint(es[2], es[3]))
    over = [t - c for t, c in zip(ts, tc)]
    sums_ref[0] += fold(log_one_plus(q4) + LN2 * ((over[0] + over[1]) + (over[2] + over[3])))
    sums_ref[1] += fold((ps[0] + ps[1]) + (ps[2] + ps[3]))
    sums_ref[2] += fold((ps[0] * dots[0] + ps[1] * dots[1]) + (ps[2] * dots[2] + ps[3] * dots[3]))
    for k in range(4):
        c_ref[:, k * quarter:(k + 1) * quarter] = ps[k].astype(jnp.bfloat16)


def txt_elem(s_ref, c_ref, a, b2, offset):
    quarter = BK // 4
    for k in range(4):
        _, t, match = logits(s_ref, k, -a, -b2, offset)
        p = 1.0 / (1.0 + jnp.exp2(t))
        if offset is not None:
            p = jnp.where(match, -p, p)
        c_ref[:, k * quarter:(k + 1) * quarter] = p.astype(jnp.bfloat16)


def kernel(coef, q0_ref, q1_ref, own0_ref, own1_ref, out0_ref, out1_ref, sums_ref, all0_ref, all1_ref, kb0, kb1, s00, s01, s10, s11, c00, c01, c10, c11, ksem, hop_send, hop_recv, pair_send, pair_recv, part_ref, gathered, sum_send, sum_recv, free):
    rows_local = q0_ref.shape[0]
    nq = rows_local // BQ
    parts = rows_local // BK
    chips = all0_ref.shape[0] // rows_local
    n_dev = 2 * chips
    nkb = n_dev * parts
    total = nkb * nq
    a, b2 = coef[0], coef[1]
    me = lax.axis_index('dp')
    core, chip = lax.rem(me, 2), lax.div(me, 2)
    partner = me + 1 - 2 * core
    owns, alls, kbs, locals_ = (own0_ref, own1_ref), (all0_ref, all1_ref), (kb0, kb1), (q1_ref, q0_ref)

    def remote(source, target, send, recv, device):
        return pltpu.make_async_remote_copy(source, target, send, recv, device_id=(device,), device_id_type=pl.DeviceIdType.MESH)

    def weights(part, side):
        result = []
        for k in range(3):
            axis = jnp.where(part == 3, 2 - k if side == 0 else k, lax.rem(part + k, 3))
            weight = 1 + axis + lax.div(axis, 2)
            result.append(weight * (1 - 2 * lax.rem(lax.div(chip, weight), 2)))
        return result

    def place(route, part, side):
        bits = (lax.rem(route, 2), lax.rem(lax.div(route, 2), 2), lax.div(route, 4))
        source = chip
        for bit, flip in zip(bits, weights(part, side)):
            source = source + bit * flip
        return pl.ds(pl.multiple_of(source * rows_local + part * BK, BK), BK)

    def message(route, part, side):
        return (route * parts + part) * 2 + side

    def local_rows(part, side):
        return locals_[side].at[pl.ds(pl.multiple_of(part * BK, BK), BK), :]

    def hop(route, k, part, side, own=False):
        index = message(route + (1 << k), part, side)
        rows = alls[side].at[place(route, part, side), :]
        return remote(local_rows(part, side) if own else rows, rows, hop_send.at[index], hop_recv.at[index], me + 2 * weights(part, side)[k])

    def hop_arrival(route, part, side):
        index = message(route, part, side)
        rows = alls[side].at[place(route, part, side), :]
        return remote(rows, rows, hop_send.at[index], hop_recv.at[index], partner)

    def pair(route, part, side, source):
        index = message(route, part, side)
        return remote(source, kbs[side].at[parts + part], pair_send.at[index], pair_recv.at[index], partner)

    def stage_of(j):
        return lax.div(j, 2 * parts)

    def route_of(j):
        i = stage_of(j)
        return i + jnp.where(i == 3, 1, 0) - jnp.where(i == 4, 1, 0)

    def part_of(j):
        return lax.rem(j, parts)

    def from_partner(j):
        return lax.rem(lax.div(j, parts), 2) == 1

    def ring(j):
        return part_of(j)

    def slot(j):
        return lax.rem(j, 2 * parts)

    def fetch_own(j):
        row = pl.multiple_of(part_of(j) * BK, BK)
        return [pltpu.make_async_copy(owns[side].at[pl.ds(row, BK), :], kbs[side].at[ring(j)], ksem.at[side, ring(j)]) for side in range(2)]

    def fetch(j):
        return [pltpu.make_async_copy(alls[side].at[place(route_of(j), part_of(j), side), :], kbs[side].at[ring(j)], ksem.at[side, ring(j)]) for side in range(2)]

    def pair_block(j, side):
        return pair(route_of(j), part_of(j), side, kbs[side].at[ring(j)])

    def make_ready(j):
        partner_block = from_partner(j)

        @pl.when(partner_block)
        def _():
            for side in range(2):
                pair_block(j, side).wait_recv()

        @pl.when(jnp.logical_not(partner_block))
        def _():
            for c in fetch(j):
                c.wait()
            pl.semaphore_wait(free.at[part_of(j)], 1)
            for side in range(2):
                pair_block(j, side).start()

    def prefetch(j):
        route, part = route_of(j), part_of(j)
        for side in range(2):
            hop_arrival(route, part, side).wait_recv()
        for k in range(1, 3):
            @pl.when(route < (1 << k))
            def _():
                for side in range(2):
                    hop(route, k, part, side).start()

        @pl.when(stage_of(j) >= 2)
        def _():
            for side in range(2):
                pair_block(j - 2 * parts, side).wait_send()
        for c in fetch(j):
            c.start()

    barrier = pltpu.get_barrier_semaphore()

    def greet(n, _):
        pl.semaphore_signal(barrier, inc=1, device_id=(lax.rem(me + n, n_dev),), device_id_type=pl.DeviceIdType.MESH)
        return 0

    lax.fori_loop(1, n_dev, greet, 0)
    for c in fetch_own(0) + fetch_own(1):
        c.start()
    pl.semaphore_wait(barrier, n_dev - 1)

    def start_own(part, _):
        for side in range(2):
            hop(0, 0, part, side, own=True).start()
        for side in range(2):
            pair(0, part, side, local_rows(part, side)).start()
        return 0

    def start_later(part, _):
        for k in range(1, 3):
            for side in range(2):
                hop(0, k, part, side, own=True).start()
        return 0

    lax.fori_loop(0, parts, start_own, 0)
    lax.fori_loop(0, parts, start_later, 0)

    part_ref[...] = jnp.zeros_like(part_ref)
    out0_ref[...] = jnp.zeros_like(out0_ref)
    out1_ref[...] = jnp.zeros_like(out1_ref)
    c01[...] = jnp.zeros_like(c01)
    c11[...] = jnp.zeros_like(c11)
    for c in fetch_own(0):
        c.wait()
    s00[...] = lax.dot_general(q0_ref[0:BQ, :], kb0[0], NT, preferred_element_type=jnp.float32)
    s10[...] = lax.dot_general(q1_ref[0:BQ, :], kb1[0], NT, preferred_element_type=jnp.float32)

    def grads(qp, sp, o, ci, kb):
        o[pl.ds(qp, BQ), :] += lax.dot_general(ci[...], kb[sp], NN, preferred_element_type=jnp.float32)

    def step(t, s0i, s0o, s1i, s1o, c0i, c0o, c1i, c1o, own):
        t_next = jnp.minimum(t + 1, total - 1)
        t_prev = jnp.maximum(t - 1, 0)
        qn = pl.multiple_of(lax.rem(t_next, nq) * BQ, BQ)
        qp = pl.multiple_of(lax.rem(t_prev, nq) * BQ, BQ)
        sn = slot(lax.div(t_next, nq))
        sp = slot(lax.div(t_prev, nq))
        offset = lax.div(t, nq) * BK - lax.rem(t, nq) * BQ if own else None
        s0o[...] = lax.dot_general(q0_ref[pl.ds(qn, BQ), :], kb0[sn], NT, preferred_element_type=jnp.float32)
        img_elem(s0i, c0o, part_ref, a, b2, offset)
        grads(qp, sp, out0_ref, c0i, kb0)
        s1o[...] = lax.dot_general(q1_ref[pl.ds(qn, BQ), :], kb1[sn], NT, preferred_element_type=jnp.float32)
        txt_elem(s1i, c1o, a, b2, offset)
        grads(qp, sp, out1_ref, c1i, kb1)

    def own_body(j, _):
        @pl.when(j + 1 < parts)
        def _():
            for c in fetch_own(j + 1):
                c.wait()

        @pl.when(j + 1 == parts)
        def _():
            for side in range(2):
                pair(0, 0, side, local_rows(0, side)).wait_recv()

        step(2 * j, s00, s01, s10, s11, c01, c00, c11, c10, True)

        @pl.when(j + 2 < parts)
        def _():
            for c in fetch_own(j + 2):
                c.start()

        step(2 * j + 1, s01, s00, s11, s10, c00, c01, c10, c11, True)
        return 0

    def body(j, _):
        @pl.when(j + 1 < nkb)
        def _():
            make_ready(j + 1)

        @pl.when(jnp.logical_and(from_partner(j - 2), j - 2 < nkb - parts))
        def _():
            pl.semaphore_signal(free.at[part_of(j - 2)], inc=1, device_id=(partner,), device_id_type=pl.DeviceIdType.MESH)

        @pl.when(jnp.logical_and(j + 2 < nkb, jnp.logical_not(from_partner(j + 2))))
        def _():
            prefetch(j + 2)

        step(2 * j, s00, s01, s10, s11, c01, c00, c11, c10, False)
        step(2 * j + 1, s01, s00, s11, s10, c00, c01, c10, c11, False)
        return 0

    lax.fori_loop(0, parts, own_body, 0)
    lax.fori_loop(parts, nkb, body, 0)
    last = slot(nkb - 1)
    grads((nq - 1) * BQ, last, out0_ref, c01, kb0)

    def share(target, sender):
        return remote(part_ref, gathered.at[sender], sum_send.at[target], sum_recv.at[sender], target)

    def share_start(n, _):
        share(lax.rem(me + n, n_dev), me).start()
        return 0

    def share_wait(n, _):
        other = lax.rem(me + n, n_dev)
        share(other, other).wait_recv()
        share(other, me).wait_send()
        return 0

    lax.fori_loop(1, n_dev, share_start, 0)
    gathered[me] = part_ref[...]
    grads((nq - 1) * BQ, last, out1_ref, c11, kb1)
    lax.fori_loop(1, n_dev, share_wait, 0)
    sums_ref[...] = jnp.sum(gathered[...], axis=0)

    def drain_hops(n, _):
        for side in range(2):
            hop_arrival(lax.div(n, parts), lax.rem(n, parts), side).wait_send()
        return 0

    def drain_first(part, _):
        for side in range(2):
            pair(0, part, side, local_rows(part, side)).wait_send()
        return 0

    def drain_last(part, _):
        for side in range(2):
            pair_block(nkb - 2 * parts + part, side).wait_send()
        return 0

    lax.fori_loop(parts, chips * parts, drain_hops, 0)
    lax.fori_loop(0, parts, drain_first, 0)
    lax.fori_loop(0, parts, drain_last, 0)


def both_sides(coef, img, txt, n_dev):
    rows, depth = img.shape
    in_vmem = pl.BlockSpec(memory_space=pltpu.VMEM)
    anywhere = pl.BlockSpec(memory_space=pl.ANY)
    grad = jax.ShapeDtypeStruct((rows, depth), jnp.float32)
    whole = jax.ShapeDtypeStruct((rows * (n_dev // 2), depth), img.dtype)
    messages = 8 * (rows // BK) * 2
    return pl.pallas_call(
        kernel,
        out_shape=(grad, grad, jax.ShapeDtypeStruct((3, 8, 128), jnp.float32), whole, whole),
        in_specs=[pl.BlockSpec(memory_space=pltpu.SMEM), in_vmem, in_vmem, anywhere, anywhere],
        out_specs=(in_vmem, in_vmem, in_vmem, anywhere, anywhere),
        scratch_shapes=[pltpu.VMEM((2 * (rows // BK), BK, depth), jnp.bfloat16)] * 2
        + [pltpu.VMEM((BQ, BK), jnp.float32)] * 4
        + [pltpu.VMEM((BQ, BK), jnp.bfloat16)] * 4
        + [pltpu.SemaphoreType.DMA((2, rows // BK))]
        + [pltpu.SemaphoreType.DMA((messages,))] * 4
        + [pltpu.VMEM((3, 8, 128), jnp.float32), pltpu.VMEM((n_dev, 3, 8, 128), jnp.float32)]
        + [pltpu.SemaphoreType.DMA((n_dev,))] * 2
        + [pltpu.SemaphoreType.REGULAR((rows // BK,))],
        compiler_params=pltpu.CompilerParams(vmem_limit_bytes=62 * 1024 * 1024, collective_id=0, has_side_effects=True),
    )(coef, img, txt, txt, img)


def solution(mesh):
    axis_name = mesh.axis_names[0]
    n_dev = mesh.shape[axis_name]

    def per_device(img, txt, log_temp, logit_bias):
        n_total = img.shape[0] * n_dev
        scale = jnp.exp(log_temp[0])
        coef = jnp.stack([scale * LOG2E, logit_bias[0] * LOG2E])
        img_sum, txt_sum, sums, _, _ = both_sides(coef, img, txt, n_dev)
        factor = scale / n_total
        totals = jnp.sum(sums, axis=(1, 2))
        return totals[0:1] / n_total, img_sum * factor, txt_sum * factor, totals[2:3] * factor, totals[1:2] / n_total

    return jax.shard_map(per_device, mesh=mesh, in_specs=(P(axis_name, None), P(axis_name, None), P(None), P(None)), out_specs=(P(None), P(axis_name, None), P(axis_name, None), P(None), P(None)), check_vma=False)
```
